128 devices in a mesh: pair: 8 (over x, core), ep: 16 (over z, y).
Axes of the slice: x: 4, y: 4, z: 4, core: 2. Of those that a mesh axis runs over, the one named last changes fastest.
Arguments:
- tokens: bfloat16 [32768, 4096], P(('pair', 'ep')), may hold values from -6 to 6
- expert_of: int32 [32768, 1], P(('pair', 'ep')), may hold values from 0 to 127, as said below
- w_gate: bfloat16 [128, 4096, 768], P(('pair', 'ep')), may hold values from -0.09375 to 0.09375
- w_up: bfloat16 [128, 4096, 768], P(('pair', 'ep')), may hold values from -0.09375 to 0.09375
- w_down: bfloat16 [128, 768, 4096], P(('pair', 'ep')), may hold values from -0.21875 to 0.21875
Outputs:
- mixed: bfloat16 [32768, 4096], P(('pair', 'ep'))
The draws below stay inside these ranges and needn't reach their ends.
Inputs may be any that keep to these rules, and one draw needn't show every extreme that they name: `expert_of`: the rows of one device (aligned blocks of 256 tokens) name no expert more than 3 times; in every draw one expert, drawn from the seed, is named exactly 3 times in every device's rows.
All inputs are finite; a program needn't handle non-finite values.
Results may differ from the reference program's by a relative error of at most 0.005.
Values may be sent and summed in bfloat16 or wider, within the bound.
No kernel may reach another device: no remote copies, remote signals or barrier semaphores. Data moves between devices by JAX's collectives and lax.ppermute only.
A program may use at most 128 MiB of HBM per device.

```python
import jax
import jax.numpy as jnp
from jax import lax

D = 4096
FF = 768
TOK_DEV = 256
EXPERTS = 128
CAP = 3
TOKENS = 32768


def draw_expert_of(key, part):
    blocks = TOKENS // TOK_DEV
    hottest = jax.random.randint(jax.random.fold_in(key, 7), (), 0, EXPERTS).astype(jnp.int32)
    block_keys = jax.random.split(jax.random.fold_in(key, 11), blocks)

    def one_block(block_key):
        first_key, second_key = jax.random.split(block_key)
        others = jnp.repeat(jnp.arange(EXPERTS - 1, dtype=jnp.int32), CAP)
        others = jax.random.permutation(first_key, others)[:TOK_DEV - CAP]
        others = others + (others >= hottest).astype(jnp.int32)
        block_rows = jnp.concatenate([jnp.full((CAP,), hottest, jnp.int32), others])
        return jax.random.permutation(second_key, block_rows)
    return jax.vmap(one_block)(block_keys).reshape(TOKENS, 1).astype(jnp.int32)


def steps_of(stream_key, dims, shards, least, high):
    def one(dim, blocks):
        steps = jax.random.uniform(jax.random.fold_in(jax.random.fold_in(stream_key, 6), dim), (blocks,), jnp.float32, least / len(shards), high / len(shards))
        return jnp.repeat(jnp.exp(steps), dims[dim] // blocks).reshape((-1,) + (1,) * (len(dims) - dim - 1))

    level = one(*shards[0])
    for cut in shards[1:]:
        level = level * one(*cut)
    return level


def normal_values(stream_key, extent, scale, bound, cuts=(), kind=jnp.bfloat16):
    values = scale * jax.random.normal(stream_key, extent, jnp.float32)
    if cuts:
        values = values * steps_of(stream_key, extent, cuts, -0.22, 0.18)
    return jnp.clip(values, -bound, bound).astype(kind)


def setup_inputs(seed: int = 0) -> dict:
    keys = jax.random.split(jax.random.key(seed), 6)
    return {
        "tokens": normal_values(keys[0], (TOKENS, D), 1.0, 6.0, ((0, 128),)),
        "expert_of": draw_expert_of(jax.random.fold_in(keys[5], 71), 0),
        "w_gate": normal_values(keys[2], (EXPERTS, D, FF), D ** -0.5, 0.09375, ((0, 128),)),
        "w_up": normal_values(keys[3], (EXPERTS, D, FF), D ** -0.5, 0.09375, ((0, 128),)),
        "w_down": normal_values(keys[4], (EXPERTS, FF, D), FF ** -0.5, 0.21875, ((0, 128),)),
    }


def reference(tokens, expert_of, w_gate, w_up, w_down):
    routed = expert_of[:, 0].astype(jnp.int32)
    row_limit = EXPERTS * CAP
    sorted_rows = jnp.argsort(routed, stable=True).astype(jnp.int32)
    expert_load = jnp.sum((routed[:, None] == jnp.arange(EXPERTS, dtype=jnp.int32)[None, :]).astype(jnp.int32), axis=0).astype(jnp.int32)
    offsets = (jnp.cumsum(expert_load) - expert_load).astype(jnp.int32)
    padded_order = jnp.concatenate([sorted_rows, jnp.full((row_limit,), TOKENS, jnp.int32)])

    def per_expert(mixed_sofar, expert):
        picked = lax.dynamic_slice(padded_order, (offsets[expert].astype(jnp.int32),), (row_limit,))
        is_live = jnp.arange(row_limit, dtype=jnp.int32) < expert_load[expert]
        picked = jnp.where(is_live, picked, TOKENS).astype(jnp.int32)
        gathered = jnp.take(tokens, jnp.minimum(picked, TOKENS - 1), axis=0)
        gate_proj = jnp.dot(gathered, w_gate[expert], preferred_element_type=jnp.float32)
        up_proj = jnp.dot(gathered, w_up[expert], preferred_element_type=jnp.float32)
        hidden = (jax.nn.silu(gate_proj) * up_proj).astype(jnp.bfloat16)
        result = jnp.dot(hidden, w_down[expert], preferred_element_type=jnp.float32).astype(jnp.bfloat16)
        return mixed_sofar.at[picked].set(result, mode="drop"), None

    start = jnp.zeros((TOKENS, D), jnp.bfloat16)
    mixed, _ = lax.scan(per_expert, start, jnp.arange(EXPERTS, dtype=jnp.int32))
    return mixed
```

```python
import functools

import jax
import jax.numpy as jnp
from jax import lax
from jax.experimental import pallas as pl
from jax.experimental.pallas import tpu as pltpu
from jax.sharding import PartitionSpec as P

SLOTS = 3
SUB = 8
GROUP = 32
BF16 = jnp.bfloat16
F32 = jnp.float32


def wire_permutation(inverse):
    size = SUB * GROUP
    row = lax.broadcasted_iota(jnp.int32, (size, size), 0)
    col = lax.broadcasted_iota(jnp.int32, (size, size), 1)
    if inverse:
        row, col = col, row
    picked = (row % GROUP) * SUB + row // GROUP
    return (picked == col).astype(F32).astype(BF16)


def dot(a, b):
    return jnp.dot(a, b, preferred_element_type=F32)


def slot_onehots(expert_row, experts):
    tokens = expert_row.shape[1]
    chosen = lax.broadcasted_iota(jnp.int32, (experts, tokens), 0) == expert_row
    earlier = (
        lax.broadcasted_iota(jnp.int32, (tokens, tokens), 0)
        < lax.broadcasted_iota(jnp.int32, (tokens, tokens), 1)
    )
    before = dot(chosen.astype(F32).astype(BF16), earlier.astype(F32).astype(BF16))
    return [
        jnp.where(chosen & (before == float(slot)), 1.0, 0.0).astype(BF16)
        for slot in range(SLOTS)
    ]


def unpack_wire(wire_ref, rows_ref):
    peers = wire_ref.shape[0] // SUB
    width = wire_ref.shape[1] // SLOTS
    size = SUB * GROUP
    perm = wire_permutation(False)
    for b in range(peers // GROUP):
        block = dot(perm, wire_ref[b * size : (b + 1) * size, :]).astype(BF16)
        for slot in range(SLOTS):
            for k in range(SUB):
                rows_ref[
                    slot * peers + b * GROUP : slot * peers + (b + 1) * GROUP,
                    k * width : (k + 1) * width,
                ] = block[k * GROUP : (k + 1) * GROUP, slot * width : (slot + 1) * width]


def stage_rows(part, k, staged_ref):
    peers = part.shape[0] // SLOTS
    width = part.shape[1]
    size = SUB * GROUP
    for b in range(peers // GROUP):
        for slot in range(SLOTS):
            staged_ref[
                b * size + k * GROUP : b * size + (k + 1) * GROUP,
                slot * width : (slot + 1) * width,
            ] = part[slot * peers + b * GROUP : slot * peers + (b + 1) * GROUP]


def pack_wire(staged_ref, wire_ref):
    size = SUB * GROUP
    perm = wire_permutation(True)
    for b in range(staged_ref.shape[0] // size):
        rows = slice(b * size, (b + 1) * size)
        wire_ref[rows, :] = dot(perm, staged_ref[rows, :]).astype(BF16)


def dispatch_kernel(experts, expert_ref, tok_hbm, wire_ref, tok_ref, staged_ref, sems):
    width = tok_ref.shape[1] // SUB
    copies = []
    for k in range(SUB):
        cols = slice(k * width, (k + 1) * width)
        copy = pltpu.make_async_copy(tok_hbm.at[:, cols], tok_ref.at[:, cols], sems.at[k])
        copy.start()
        copies.append(copy)
    onehot = jnp.concatenate(slot_onehots(expert_ref[...], experts), axis=0)
    for k in range(SUB):
        copies[k].wait()
        part = dot(onehot, tok_ref[:, k * width : (k + 1) * width]).astype(BF16)
        stage_rows(part, k, staged_ref)
    pack_wire(staged_ref, wire_ref)


def ffn_kernel(wire_ref, gate_ref, up_ref, down_ref, out_ref, rows_ref, hidden_ref, staged_ref):
    unpack_wire(wire_ref, rows_ref)
    ff = gate_ref.shape[1]
    step = 256

    def hidden_block(i, _):
        cols = pl.ds(pl.multiple_of(i * step, step), step)
        gate = dot(rows_ref[...], gate_ref[:, cols])
        up = dot(rows_ref[...], up_ref[:, cols])
        hidden_ref[:, cols] = (gate / (1.0 + jnp.exp(-gate)) * up).astype(BF16)
        return 0

    lax.fori_loop(0, ff // step, hidden_block, 0)
    width = down_ref.shape[1] // SUB
    for k in range(SUB):
        part = dot(hidden_ref[...], down_ref[:, k * width : (k + 1) * width]).astype(BF16)
        stage_rows(part, k, staged_ref)
    pack_wire(staged_ref, out_ref)


def combine_kernel(experts, expert_ref, wire_ref, out_hbm, rows_ref, out_ref, sems):
    onehot = jnp.concatenate(slot_onehots(expert_ref[...], experts), axis=0)
    pick = onehot.astype(F32).T.astype(BF16)
    unpack_wire(wire_ref, rows_ref)
    width = out_ref.shape[1] // SUB
    copies = []
    for k in range(SUB):
        cols = slice(k * width, (k + 1) * width)
        out_ref[:, cols] = dot(pick, rows_ref[:, cols]).astype(BF16)
        copy = pltpu.make_async_copy(out_ref.at[:, cols], out_hbm.at[:, cols], sems.at[k])
        copy.start()
        copies.append(copy)
    for copy in copies:
        copy.wait()


VMEM = pl.BlockSpec(memory_space=pltpu.VMEM)
ANY = pl.BlockSpec(memory_space=pl.ANY)
HBM = pl.BlockSpec(memory_space=pltpu.HBM)


def shards(tokens, expert_of, w_gate, w_up, w_down):
    axes = ("pair", "ep")
    experts = lax.axis_size("pair") * lax.axis_size("ep")
    tok_rows, d = tokens.shape
    ff = w_gate.shape[2]
    wire_shape = (experts * SUB, SLOTS * d // SUB)
    wire = jax.ShapeDtypeStruct(wire_shape, BF16)
    expert_row = expert_of.reshape(1, tok_rows)

    def exchange(x):
        x = x.reshape(experts, SUB, x.shape[1])
        x = lax.all_to_all(x, axes, split_axis=0, concat_axis=0, tiled=True)
        return x.reshape(wire_shape)

    outgoing = pl.pallas_call(
        functools.partial(dispatch_kernel, experts),
        out_shape=wire,
        in_specs=[VMEM, HBM],
        out_specs=VMEM,
        scratch_shapes=[
            pltpu.VMEM((tok_rows, d), BF16),
            pltpu.VMEM(wire_shape, BF16),
            pltpu.SemaphoreType.DMA((SUB,)),
        ],
        name="dispatch",
    )(expert_row, tokens)
    arrived = exchange(outgoing)
    result = pl.pallas_call(
        ffn_kernel,
        out_shape=wire,
        in_specs=[VMEM] * 4,
        out_specs=VMEM,
        scratch_shapes=[
            pltpu.VMEM((SLOTS * experts, d), BF16),
            pltpu.VMEM((SLOTS * experts, ff), BF16),
            pltpu.VMEM(wire_shape, BF16),
        ],
        compiler_params=pltpu.CompilerParams(vmem_limit_bytes=28 * 2**20),
        name="ffn",
    )(arrived, w_gate[0], w_up[0], w_down[0])
    returned = exchange(result)
    return pl.pallas_call(
        functools.partial(combine_kernel, experts),
        out_shape=jax.ShapeDtypeStruct((tok_rows, d), BF16),
        in_specs=[VMEM, VMEM],
        out_specs=HBM,
        scratch_shapes=[
            pltpu.VMEM((SLOTS * experts, d), BF16),
            pltpu.VMEM((tok_rows, d), BF16),
            pltpu.SemaphoreType.DMA((SUB,)),
        ],
        name="combine",
    )(expert_row, returned)


def solution(mesh):
    spec = P(("pair", "ep"), None)
    weights = P(("pair", "ep"), None, None)
    return jax.shard_map(
        shards,
        mesh=mesh,
        in_specs=(spec, spec, weights, weights, weights),
        out_specs=spec,
        check_vma=False,
    )
```

```python
import functools

import jax
import jax.numpy as jnp
from jax import lax
from jax.experimental import pallas as pl
from jax.experimental.pallas import tpu as pltpu
from jax.sharding import PartitionSpec as P

SLOTS = 3
SUB = 8
GROUP = 32
BF16 = jnp.bfloat16
F32 = jnp.float32


def wire_permutation(inverse):
    size = SUB * GROUP
    row = lax.broadcasted_iota(jnp.int32, (size, size), 0)
    col = lax.broadcasted_iota(jnp.int32, (size, size), 1)
    if inverse:
        row, col = col, row
    picked = (row % GROUP) * SUB + row // GROUP
    return (picked == col).astype(F32).astype(BF16)


def dot(a, b):
    return jnp.dot(a, b, preferred_element_type=F32)


def slot_onehots(expert_row, experts):
    tokens = expert_row.shape[1]
    chosen = lax.broadcasted_iota(jnp.int32, (experts, tokens), 0) == expert_row
    earlier = (
        lax.broadcasted_iota(jnp.int32, (tokens, tokens), 0)
        < lax.broadcasted_iota(jnp.int32, (tokens, tokens), 1)
    )
    before = dot(chosen.astype(F32).astype(BF16), earlier.astype(F32).astype(BF16))
    return [
        jnp.where(chosen & (before == float(slot)), 1.0, 0.0)
        for slot in range(SLOTS)
    ]


def unpack_wire(wire_ref, rows_ref):
    peers = wire_ref.shape[0] // SUB
    width = wire_ref.shape[1] // SLOTS
    size = SUB * GROUP
    perm = wire_permutation(False)
    for b in range(peers // GROUP):
        block = dot(perm, wire_ref[b * size : (b + 1) * size, :]).astype(BF16)
        for slot in range(SLOTS):
            for k in range(SUB):
                rows_ref[
                    slot * peers + b * GROUP : slot * peers + (b + 1) * GROUP,
                    k * width : (k + 1) * width,
                ] = block[k * GROUP : (k + 1) * GROUP, slot * width : (slot + 1) * width]


def stage_rows(part, k, staged_ref):
    peers = part.shape[0] // SLOTS
    width = part.shape[1]
    size = SUB * GROUP
    for b in range(peers // GROUP):
        for slot in range(SLOTS):
            staged_ref[
                b * size + k * GROUP : b * size + (k + 1) * GROUP,
                slot * width : (slot + 1) * width,
            ] = part[slot * peers + b * GROUP : slot * peers + (b + 1) * GROUP]


def pack_wire(staged_ref, wire_ref):
    size = SUB * GROUP
    perm = wire_permutation(True)
    for b in range(staged_ref.shape[0] // size):
        rows = slice(b * size, (b + 1) * size)
        wire_ref[rows, :] = dot(perm, staged_ref[rows, :]).astype(BF16)


def dispatch_kernel(
    experts, expert_hbm, tok_hbm, wire_ref, pick_ref, expert_ref, tok_ref, staged_ref, sems
):
    width = tok_ref.shape[1] // SUB
    expert_copy = pltpu.make_async_copy(expert_hbm, expert_ref, sems.at[SUB])
    expert_copy.start()
    copies = []
    for k in range(SUB):
        cols = slice(k * width, (k + 1) * width)
        copy = pltpu.make_async_copy(tok_hbm.at[:, cols], tok_ref.at[:, cols], sems.at[k])
        copy.start()
        copies.append(copy)
    expert_copy.wait()
    onehot = jnp.concatenate(slot_onehots(expert_ref[...], experts), axis=0)
    pick_ref[...] = onehot.T.astype(BF16)
    onehot = onehot.astype(BF16)
    for k in range(SUB):
        copies[k].wait()
        part = dot(onehot, tok_ref[:, k * width : (k + 1) * width]).astype(BF16)
        stage_rows(part, k, staged_ref)
    pack_wire(staged_ref, wire_ref)


def ffn_kernel(
    wire_ref,
    gate_ref,
    up_hbm,
    down_hbm,
    out_ref,
    rows_ref,
    act_ref,
    hidden_ref,
    staged_ref,
    up_ref,
    down_ref,
    sems,
):
    up_copy = pltpu.make_async_copy(up_hbm, up_ref, sems.at[0])
    down_copy = pltpu.make_async_copy(down_hbm, down_ref, sems.at[1])
    up_copy.start()
    down_copy.start()
    unpack_wire(wire_ref, rows_ref)
    ff = gate_ref.shape[1]
    step = 256
    for i in range(ff // step):
        cols = slice(i * step, (i + 1) * step)
        gate = dot(rows_ref[...], gate_ref[:, cols])
        act_ref[:, cols] = gate / (1.0 + jnp.exp(-gate))
    up_copy.wait()
    for i in range(ff // step):
        cols = slice(i * step, (i + 1) * step)
        up = dot(rows_ref[...], up_ref[:, cols])
        hidden_ref[:, cols] = (act_ref[:, cols] * up).astype(BF16)
    down_copy.wait()
    width = down_ref.shape[1] // SUB
    for k in range(SUB):
        part = dot(hidden_ref[...], down_ref[:, k * width : (k + 1) * width]).astype(BF16)
        stage_rows(part, k, staged_ref)
    pack_wire(staged_ref, out_ref)


def combine_kernel(pick_ref, wire_ref, out_hbm, rows_ref, out_ref, sems):
    unpack_wire(wire_ref, rows_ref)
    width = out_ref.shape[1] // SUB
    copies = []
    for k in range(SUB):
        cols = slice(k * width, (k + 1) * width)
        out_ref[:, cols] = dot(pick_ref[...], rows_ref[:, cols]).astype(BF16)
        copy = pltpu.make_async_copy(out_ref.at[:, cols], out_hbm.at[:, cols], sems.at[k])
        copy.start()
        copies.append(copy)
    for copy in copies:
        copy.wait()


VMEM = pl.BlockSpec(memory_space=pltpu.VMEM)
HBM = pl.BlockSpec(memory_space=pltpu.HBM)
SMALL = pltpu.CompilerParams(vmem_limit_bytes=16 * 2**20)


def in_hbm(x):
    return pltpu.with_memory_space_constraint(x, pltpu.HBM)


def shards(tokens, expert_of, w_gate, w_up, w_down):
    axes = ("pair", "ep")
    experts = lax.axis_size("pair") * lax.axis_size("ep")
    tok_rows, d = tokens.shape
    ff = w_gate.shape[2]
    wire_shape = (experts * SUB, SLOTS * d // SUB)
    wire = pltpu.VMEM(wire_shape, BF16)
    expert_row = expert_of.reshape(1, tok_rows)

    def exchange(x):
        x = x.reshape(experts, SUB, x.shape[1])
        x = lax.all_to_all(x, axes, split_axis=0, concat_axis=0, tiled=True)
        return x.reshape(wire_shape)

    outgoing, pick = pl.pallas_call(
        functools.partial(dispatch_kernel, experts),
        out_shape=(wire, jax.ShapeDtypeStruct((tok_rows, SLOTS * experts), BF16)),
        in_specs=[HBM, HBM],
        out_specs=(VMEM, VMEM),
        scratch_shapes=[
            pltpu.VMEM((1, tok_rows), jnp.int32),
            pltpu.VMEM((tok_rows, d), BF16),
            pltpu.VMEM(wire_shape, BF16),
            pltpu.SemaphoreType.DMA((SUB + 1,)),
        ],
        compiler_params=SMALL,
        name="dispatch",
    )(in_hbm(expert_row), in_hbm(tokens))
    arrived = exchange(outgoing)
    result = pl.pallas_call(
        ffn_kernel,
        out_shape=wire,
        in_specs=[VMEM, VMEM, HBM, HBM],
        out_specs=VMEM,
        scratch_shapes=[
            pltpu.VMEM((SLOTS * experts, d), BF16),
            pltpu.VMEM((SLOTS * experts, ff), F32),
            pltpu.VMEM((SLOTS * experts, ff), BF16),
            pltpu.VMEM(wire_shape, BF16),
            pltpu.VMEM((d, ff), BF16),
            pltpu.VMEM((ff, d), BF16),
            pltpu.SemaphoreType.DMA((2,)),
        ],
        compiler_params=pltpu.CompilerParams(vmem_limit_bytes=28 * 2**20),
        name="ffn",
    )(arrived, w_gate[0], in_hbm(w_up[0]), in_hbm(w_down[0]))
    returned = exchange(result)
    return pl.pallas_call(
        combine_kernel,
        out_shape=jax.ShapeDtypeStruct((tok_rows, d), BF16),
        in_specs=[VMEM, VMEM],
        out_specs=HBM,
        scratch_shapes=[
            pltpu.VMEM((SLOTS * experts, d), BF16),
            pltpu.VMEM((tok_rows, d), BF16),
            pltpu.SemaphoreType.DMA((SUB,)),
        ],
        compiler_params=SMALL,
        name="combine",
    )(pick, returned)


def solution(mesh):
    spec = P(("pair", "ep"), None)
    weights = P(("pair", "ep"), None, None)
    return jax.shard_map(
        shards,
        mesh=mesh,
        in_specs=(spec, spec, weights, weights, weights),
        out_specs=spec,
        check_vma=False,
    )
```

```python
import functools

import jax
import jax.numpy as jnp
from jax import lax
from jax.experimental import pallas as pl
from jax.experimental.pallas import tpu as pltpu
from jax.sharding import PartitionSpec as P

SLOTS = 3
SUB = 8
GROUP = 32
BF16 = jnp.bfloat16
F32 = jnp.float32


def wire_permutation(inverse):
    size = SUB * GROUP
    row = lax.broadcasted_iota(jnp.int32, (size, size), 0)
    col = lax.broadcasted_iota(jnp.int32, (size, size), 1)
    if inverse:
        row, col = col, row
    picked = (row % GROUP) * SUB + row // GROUP
    return (picked == col).astype(F32).astype(BF16)


def dot(a, b):
    return jnp.dot(a, b, preferred_element_type=F32)


def slot_onehots(expert_row, experts):
    tokens = expert_row.shape[1]
    chosen = lax.broadcasted_iota(jnp.int32, (experts, tokens), 0) == expert_row
    earlier = (
        lax.broadcasted_iota(jnp.int32, (tokens, tokens), 0)
        < lax.broadcasted_iota(jnp.int32, (tokens, tokens), 1)
    )
    before = dot(chosen.astype(F32).astype(BF16), earlier.astype(F32).astype(BF16))
    return [
        jnp.where(chosen & (before == float(slot)), 1.0, 0.0)
        for slot in range(SLOTS)
    ]


def unpack_wire(wire_ref, rows_ref):
    peers = wire_ref.shape[0] // SUB
    width = wire_ref.shape[1] // SLOTS
    size = SUB * GROUP
    perm = wire_permutation(False)
    for b in range(peers // GROUP):
        block = dot(perm, wire_ref[b * size : (b + 1) * size, :]).astype(BF16)
        for slot in range(SLOTS):
            for k in range(SUB):
                rows_ref[
                    slot * peers + b * GROUP : slot * peers + (b + 1) * GROUP,
                    k * width : (k + 1) * width,
                ] = block[k * GROUP : (k + 1) * GROUP, slot * width : (slot + 1) * width]


def stage_rows(part, k, staged_ref):
    peers = part.shape[0] // SLOTS
    width = part.shape[1]
    size = SUB * GROUP
    for b in range(peers // GROUP):
        for slot in range(SLOTS):
            staged_ref[
                b * size + k * GROUP : b * size + (k + 1) * GROUP,
                slot * width : (slot + 1) * width,
            ] = part[slot * peers + b * GROUP : slot * peers + (b + 1) * GROUP]


def pack_wire(staged_ref, wire_ref):
    size = SUB * GROUP
    perm = wire_permutation(True)
    for b in range(staged_ref.shape[0] // size):
        rows = slice(b * size, (b + 1) * size)
        wire_ref[rows, :] = dot(perm, staged_ref[rows, :]).astype(BF16)


def dispatch_kernel(
    experts, expert_hbm, tok_hbm, wire_ref, pick_ref, expert_ref, tok_ref, staged_ref, sems
):
    width = tok_ref.shape[1] // SUB
    expert_copy = pltpu.make_async_copy(expert_hbm, expert_ref, sems.at[SUB])
    expert_copy.start()
    copies = []
    for k in range(SUB):
        cols = slice(k * width, (k + 1) * width)
        copy = pltpu.make_async_copy(tok_hbm.at[:, cols], tok_ref.at[:, cols], sems.at[k])
        copy.start()
        copies.append(copy)
    expert_copy.wait()
    onehot = jnp.concatenate(slot_onehots(expert_ref[...], experts), axis=0)
    pick_ref[...] = onehot.T.astype(BF16)
    onehot = onehot.astype(BF16)
    for k in range(SUB):
        copies[k].wait()
        part = dot(onehot, tok_ref[:, k * width : (k + 1) * width]).astype(BF16)
        stage_rows(part, k, staged_ref)
    pack_wire(staged_ref, wire_ref)


def ffn_kernel(
    wire_ref,
    gate_ref,
    up_ref,
    down_ref,
    out_ref,
    rows_ref,
    act_ref,
    hidden_ref,
    staged_ref,
):
    unpack_wire(wire_ref, rows_ref)
    ff = gate_ref.shape[1]
    step = 256
    for i in range(ff // step):
        cols = slice(i * step, (i + 1) * step)
        gate = dot(rows_ref[...], gate_ref[:, cols])
        act_ref[:, cols] = gate / (1.0 + jnp.exp(-gate))
    for i in range(ff // step):
        cols = slice(i * step, (i + 1) * step)
        up = dot(rows_ref[...], up_ref[:, cols])
        hidden_ref[:, cols] = (act_ref[:, cols] * up).astype(BF16)
    width = down_ref.shape[1] // SUB
    for k in range(SUB):
        part = dot(hidden_ref[...], down_ref[:, k * width : (k + 1) * width]).astype(BF16)
        stage_rows(part, k, staged_ref)
    pack_wire(staged_ref, out_ref)


def combine_kernel(pick_ref, wire_ref, out_hbm, rows_ref, out_ref, sems):
    unpack_wire(wire_ref, rows_ref)
    width = out_ref.shape[1] // SUB
    copies = []
    for k in range(SUB):
        cols = slice(k * width, (k + 1) * width)
        out_ref[:, cols] = dot(pick_ref[...], rows_ref[:, cols]).astype(BF16)
        copy = pltpu.make_async_copy(out_ref.at[:, cols], out_hbm.at[:, cols], sems.at[k])
        copy.start()
        copies.append(copy)
    for copy in copies:
        copy.wait()


VMEM = pl.BlockSpec(memory_space=pltpu.VMEM)
HBM = pl.BlockSpec(memory_space=pltpu.HBM)
SMALL = pltpu.CompilerParams(vmem_limit_bytes=16 * 2**20)


def in_hbm(x):
    return pltpu.with_memory_space_constraint(x, pltpu.HBM)


def shards(tokens, expert_of, w_gate, w_up, w_down):
    axes = ("pair", "ep")
    experts = lax.axis_size("pair") * lax.axis_size("ep")
    tok_rows, d = tokens.shape
    ff = w_gate.shape[2]
    wire_shape = (experts * SUB, SLOTS * d // SUB)
    wire = pltpu.VMEM(wire_shape, BF16)
    expert_row = expert_of.reshape(1, tok_rows)

    def exchange(x):
        x = x.reshape(experts, SUB, x.shape[1])
        x = lax.all_to_all(x, axes, split_axis=0, concat_axis=0, tiled=True)
        return x.reshape(wire_shape)

    outgoing, pick = pl.pallas_call(
        functools.partial(dispatch_kernel, experts),
        out_shape=(wire, jax.ShapeDtypeStruct((tok_rows, SLOTS * experts), BF16)),
        in_specs=[HBM, HBM],
        out_specs=(VMEM, VMEM),
        scratch_shapes=[
            pltpu.VMEM((1, tok_rows), jnp.int32),
            pltpu.VMEM((tok_rows, d), BF16),
            pltpu.VMEM(wire_shape, BF16),
            pltpu.SemaphoreType.DMA((SUB + 1,)),
        ],
        compiler_params=SMALL,
        cost_estimate=pl.CostEstimate(flops=40 * 10**9, bytes_accessed=10**6, transcendentals=0),
        name="dispatch",
    )(in_hbm(expert_row), in_hbm(tokens))
    arrived = exchange(outgoing)
    result = pl.pallas_call(
        ffn_kernel,
        out_shape=wire,
        in_specs=[VMEM, VMEM, VMEM, VMEM],
        out_specs=VMEM,
        scratch_shapes=[
            pltpu.VMEM((SLOTS * experts, d), BF16),
            pltpu.VMEM((SLOTS * experts, ff), F32),
            pltpu.VMEM((SLOTS * experts, ff), BF16),
            pltpu.VMEM(wire_shape, BF16),
        ],
        compiler_params=pltpu.CompilerParams(vmem_limit_bytes=28 * 2**20),
        name="ffn",
    )(arrived, w_gate[0], w_up[0], w_down[0])
    returned = exchange(result)
    return pl.pallas_call(
        combine_kernel,
        out_shape=jax.ShapeDtypeStruct((tok_rows, d), BF16),
        in_specs=[VMEM, VMEM],
        out_specs=HBM,
        scratch_shapes=[
            pltpu.VMEM((SLOTS * experts, d), BF16),
            pltpu.VMEM((tok_rows, d), BF16),
            pltpu.SemaphoreType.DMA((SUB,)),
        ],
        compiler_params=SMALL,
        name="combine",
    )(pick, returned)


def solution(mesh):
    spec = P(("pair", "ep"), None)
    weights = P(("pair", "ep"), None, None)
    return jax.shard_map(
        shards,
        mesh=mesh,
        in_specs=(spec, spec, weights, weights, weights),
        out_specs=spec,
        check_vma=False,
    )
```

```python
import functools

import jax
import jax.numpy as jnp
from jax import lax
from jax.experimental import pallas as pl
from jax.experimental.pallas import tpu as pltpu
from jax.sharding import PartitionSpec as P

SLOTS = 3
SUB = 8
LANES = 128
GROUP = 32
BF16 = jnp.bfloat16
F32 = jnp.float32


def wire_permutation(inverse):
    size = SUB * GROUP
    row = lax.broadcasted_iota(jnp.int32, (size, size), 0)
    col = lax.broadcasted_iota(jnp.int32, (size, size), 1)
    if inverse:
        row, col = col, row
    picked = (row % GROUP) * SUB + row // GROUP
    return (picked == col).astype(F32).astype(BF16)


def dot(a, b):
    return jnp.dot(a, b, preferred_element_type=F32)


def slot_onehots(expert_row, experts):
    tokens = expert_row.shape[1]
    chosen = lax.broadcasted_iota(jnp.int32, (experts, tokens), 0) == expert_row
    earlier = (
        lax.broadcasted_iota(jnp.int32, (tokens, tokens), 0)
        < lax.broadcasted_iota(jnp.int32, (tokens, tokens), 1)
    )
    before = dot(chosen.astype(F32).astype(BF16), earlier.astype(F32).astype(BF16))
    return [
        jnp.where(chosen & (before == float(slot)), 1.0, 0.0)
        for slot in range(SLOTS)
    ]


def unpack_wire(wire_ref, rows_ref):
    peers = wire_ref.shape[0] // SUB
    width = wire_ref.shape[1] // SLOTS
    size = SUB * GROUP
    perm = wire_permutation(False)
    for b in range(peers // GROUP):
        block = dot(perm, wire_ref[b * size : (b + 1) * size, :]).astype(BF16)
        for slot in range(SLOTS):
            for k in range(SUB):
                rows_ref[
                    slot * peers + b * GROUP : slot * peers + (b + 1) * GROUP,
                    k * width : (k + 1) * width,
                ] = block[k * GROUP : (k + 1) * GROUP, slot * width : (slot + 1) * width]


def stage_rows(part, k, staged_ref):
    peers = part.shape[0] // SLOTS
    width = part.shape[1]
    size = SUB * GROUP
    for b in range(peers // GROUP):
        for slot in range(SLOTS):
            staged_ref[
                b * size + k * GROUP : b * size + (k + 1) * GROUP,
                slot * width : (slot + 1) * width,
            ] = part[slot * peers + b * GROUP : slot * peers + (b + 1) * GROUP]


def spread_rows(part, k, spread_ref):
    peers = part.shape[0] // SLOTS
    tiles = part.shape[1] // LANES
    for slot in range(SLOTS):
        for tile in range(tiles):
            spread_ref[slot * tiles + tile, pl.ds(k, peers, stride=SUB), :] = part[
                slot * peers : (slot + 1) * peers, tile * LANES : (tile + 1) * LANES
            ]


def narrow_rows(spread_ref, wire_ref, first, width):
    full = wire_ref.shape[1] // SLOTS
    tiles = width // LANES
    for slot in range(SLOTS):
        for tile in range(tiles):
            start = slot * full + first + tile * LANES
            wire_ref[:, start : start + LANES] = spread_ref[slot * tiles + tile].astype(BF16)


def pack_wire(staged_ref, wire_ref):
    size = SUB * GROUP
    perm = wire_permutation(True)
    for b in range(staged_ref.shape[0] // size):
        rows = slice(b * size, (b + 1) * size)
        wire_ref[rows, :] = dot(perm, staged_ref[rows, :]).astype(BF16)


def dispatch_kernel(
    experts, expert_hbm, tok_hbm, wire_ref, pick_ref, expert_ref, tok_ref, staged_ref, sems
):
    width = tok_ref.shape[1] // SUB
    expert_copy = pltpu.make_async_copy(expert_hbm, expert_ref, sems.at[SUB])
    expert_copy.start()
    copies = []
    part = tok_ref.shape[0] // SUB
    for k in range(SUB):
        rows = slice(k * part, (k + 1) * part)
        copy = pltpu.make_async_copy(tok_hbm.at[rows], tok_ref.at[rows], sems.at[k])
        copy.start()
        copies.append(copy)
    expert_copy.wait()
    onehot = jnp.concatenate(slot_onehots(expert_ref[...], experts), axis=0)
    pick_ref[...] = onehot.T.astype(BF16)
    onehot = onehot.astype(BF16)
    for copy in copies:
        copy.wait()
    half = width // 2
    for h in range(2):
        for k in range(SUB):
            first = k * width + h * half
            spread_rows(dot(onehot, tok_ref[:, first : first + half]), k, staged_ref.at[h])
        narrow_rows(staged_ref.at[h], wire_ref, h * half, half)


def ffn_kernel(
    wire_ref,
    gate_ref,
    up_ref,
    down_ref,
    out_ref,
    rows_ref,
    hidden_ref,
    staged_ref,
):
    unpack_wire(wire_ref, rows_ref)
    ff = gate_ref.shape[1]
    step = 256
    for i in range(ff // step):
        cols = slice(i * step, (i + 1) * step)
        gate = dot(rows_ref[...], gate_ref[:, cols])
        up = dot(rows_ref[...], up_ref[:, cols])
        hidden_ref[:, cols] = (gate / (1.0 + jnp.exp(-gate)) * up).astype(BF16)
    width = down_ref.shape[1] // SUB
    half = width // 2
    for h in range(2):
        for k in range(SUB):
            first = k * width + h * half
            part = dot(hidden_ref[...], down_ref[:, first : first + half])
            spread_rows(part, k, staged_ref.at[h])
        narrow_rows(staged_ref.at[h], out_ref, h * half, half)


def combine_kernel(pick_ref, wire_ref, out_hbm, rows_ref, out_ref, sems):
    unpack_wire(wire_ref, rows_ref)
    width = out_ref.shape[1] // SUB
    copies = []
    for k in range(SUB):
        cols = slice(k * width, (k + 1) * width)
        out_ref[:, cols] = dot(pick_ref[...], rows_ref[:, cols]).astype(BF16)
        copy = pltpu.make_async_copy(out_ref.at[:, cols], out_hbm.at[:, cols], sems.at[k])
        copy.start()
        copies.append(copy)
    for copy in copies:
        copy.wait()


VMEM = pl.BlockSpec(memory_space=pltpu.VMEM)
HBM = pl.BlockSpec(memory_space=pltpu.HBM)
SMALL = pltpu.CompilerParams(vmem_limit_bytes=20 * 2**20)


def in_hbm(x):
    return pltpu.with_memory_space_constraint(x, pltpu.HBM)


def shards(tokens, expert_of, w_gate, w_up, w_down):
    axes = ("pair", "ep")
    experts = lax.axis_size("pair") * lax.axis_size("ep")
    tok_rows, d = tokens.shape
    ff = w_gate.shape[2]
    wire_shape = (experts * SUB, SLOTS * d // SUB)
    wire = pltpu.VMEM(wire_shape, BF16)
    expert_row = expert_of.reshape(1, tok_rows)

    def exchange(x):
        x = x.reshape(experts, SUB, x.shape[1])
        x = lax.all_to_all(x, axes, split_axis=0, concat_axis=0, tiled=True)
        return x.reshape(wire_shape)

    outgoing, pick = pl.pallas_call(
        functools.partial(dispatch_kernel, experts),
        out_shape=(wire, jax.ShapeDtypeStruct((tok_rows, SLOTS * experts), BF16)),
        in_specs=[HBM, HBM],
        out_specs=(VMEM, VMEM),
        scratch_shapes=[
            pltpu.VMEM((1, tok_rows), jnp.int32),
            pltpu.VMEM((tok_rows, d), BF16),
            pltpu.VMEM((2, d // SUB // 2 // LANES * SLOTS, experts * SUB, LANES), F32),
            pltpu.SemaphoreType.DMA((SUB + 1,)),
        ],
        compiler_params=SMALL,
        cost_estimate=pl.CostEstimate(flops=40 * 10**9, bytes_accessed=10**6, transcendentals=0),
        name="dispatch",
    )(in_hbm(expert_row), in_hbm(tokens))
    arrived = exchange(outgoing)
    result = pl.pallas_call(
        ffn_kernel,
        out_shape=wire,
        in_specs=[VMEM, VMEM, VMEM, VMEM],
        out_specs=VMEM,
        scratch_shapes=[
            pltpu.VMEM((SLOTS * experts, d), BF16),
            pltpu.VMEM((SLOTS * experts, ff), BF16),
            pltpu.VMEM((2, d // SUB // 2 // LANES * SLOTS, experts * SUB, LANES), F32),
        ],
        compiler_params=pltpu.CompilerParams(vmem_limit_bytes=28 * 2**20),
        name="ffn",
    )(arrived, w_gate[0], w_up[0], w_down[0])
    returned = exchange(result)
    return pl.pallas_call(
        combine_kernel,
        out_shape=jax.ShapeDtypeStruct((tok_rows, d), BF16),
        in_specs=[VMEM, VMEM],
        out_specs=HBM,
        scratch_shapes=[
            pltpu.VMEM((SLOTS * experts, d), BF16),
            pltpu.VMEM((tok_rows, d), BF16),
            pltpu.SemaphoreType.DMA((SUB,)),
        ],
        compiler_params=SMALL,
        name="combine",
    )(pick, returned)


def solution(mesh):
    spec = P(("pair", "ep"), None)
    weights = P(("pair", "ep"), None, None)
    return jax.shard_map(
        shards,
        mesh=mesh,
        in_specs=(spec, spec, weights, weights, weights),
        out_specs=spec,
        check_vma=False,
    )
```
